256 devices in a mesh: grp: 2 (over y), sub: 128 (over z, x, core).
Axes of the slice: x: 4, y: 2, z: 16, core: 2. Of those that a mesh axis runs over, the one named last changes fastest.
The devices are a block of a 4x16x16 slice.
Arguments:
- factors: bfloat16 [768, 1024, 1024], P(('grp', 'sub')), parts along dimension 0, may hold values from -0.1875 to 0.1875
- coupling: bfloat16 [768, 1024, 512], P(('grp', 'sub')), parts along dimension 0, may hold values from -0.1875 to 0.1875
- gap_loads: bfloat16 [768, 512, 256], P(('grp', 'sub')), parts along dimension 0, may hold values from -6 to 6
- dof_blocks: int32 [768], P(('grp', 'sub')), parts along dimension 0, may hold values from 4 to 8, as said below
- partner_rows: int32 [768, 512], P(('grp', 'sub')), parts along dimension 0, may hold values from 0 to 196607, as said below
Outputs:
- multipliers: float32 [768, 512, 256], P(('grp', 'sub')), parts along dimension 0
- dual_residual: float32 [768, 512, 256], P(('grp', 'sub')), parts along dimension 0
- residual_rms: float32 [512], P('grp'), parts along dimension 0
The draws below stay inside these ranges and needn't reach their ends.
There are 2 independent parts, one for each index of `grp`. The reference program is written for one: setup_inputs(seed, part) draws one part's arguments, and reference() takes and returns one part's arrays. A program takes and returns all parts, laid end to end along the dimension named above; each array names one. Nothing has to cross between parts.
Inputs may be any that keep to these rules, and one draw needn't show every extreme that they name: `partner_rows`: every interface row is tied to exactly one row of a subdomain on another device, and that row is tied back to it. The rows of one device are tied to at most 16 rows of any one other device, and some pair of devices reaches that number in every draw. `dof_blocks`: some subdomain has all 1024 degrees of freedom present in every draw.
All inputs are finite; a program needn't handle non-finite values.
Results may differ from the reference program's by a relative error of at most 0.008.
Values may be sent and summed in bfloat16 or wider, within the bound.
No kernel may reach another device: no remote copies, remote signals or barrier semaphores. Data moves between devices by JAX's collectives and lax.ppermute only.
A program may use at most 64 MiB of HBM per device.

```python
import jax
import jax.numpy as jnp
from jax import lax

NDOF = 1024
IF = 512
DBLK = 128
FROWS = 16
NRHS = 256
ITERS = 3
SUB_DEV = 3
SUBS = 384
N_SUB = 128


def draw_gap_loads(key, part):
    subdomains = SUB_DEV * N_SUB
    first_key = jax.random.fold_in(key, 0)
    rising = (jnp.arange(subdomains, dtype=jnp.float32) / subdomains)[:, None, None]
    values = jnp.clip(jax.random.normal(first_key, (subdomains, IF, NRHS), jnp.float32), -4.0, 4.0) * (0.5 + rising)
    return values.astype(jnp.bfloat16)


def draw_dof_blocks(key, part):
    subdomains = SUB_DEV * N_SUB
    lowest = IF // DBLK
    highest = NDOF // DBLK
    first_key, second_key, third_key = jax.random.split(key, 3)
    extra = jax.random.randint(first_key, (subdomains,), 0, highest - lowest + 1)
    heavy = jax.random.randint(second_key, (subdomains,), 0, 2)
    blocks = lowest + extra * heavy
    chosen = jax.random.randint(third_key, (), 0, subdomains)
    blocks = jnp.where(jnp.arange(subdomains) == chosen, highest, blocks)
    return blocks.astype(jnp.int32)


def draw_partner_rows(key, part):
    row_count = SUB_DEV * IF
    faces = row_count // FROWS
    spread = max(N_SUB // 2 - 1, 1)
    first_key, second_key, third_key = jax.random.split(key, 3)
    labels = jax.random.permutation(first_key, N_SUB).astype(jnp.int32)
    holders = jnp.argsort(labels).astype(jnp.int32)
    scores = jax.random.randint(second_key, (N_SUB, faces), 0, 1 << 20) * faces + jnp.arange(faces, dtype=jnp.int32)[None, :]
    shuffle = jnp.argsort(scores, axis=1).astype(jnp.int32)
    logical = jnp.arange(faces, dtype=jnp.int32)
    offsets = 1 + logical // 2 % spread
    upward = logical % 2 == 0
    moved = jnp.where(upward, offsets, -offsets)
    other_label = (labels[:, None] + moved[None, :]) % N_SUB
    others = holders[other_label]
    other_logical = logical + 1 - 2 * (logical % 2)
    other_face = shuffle[others, other_logical[None, :]]
    even_label = jnp.where(upward[None, :], labels[:, None], other_label)
    pair_index = even_label * (faces // 2) + logical[None, :] // 2
    turns = jax.random.randint(third_key, (N_SUB * (faces // 2),), 0, FROWS)[pair_index]
    within = jnp.arange(FROWS, dtype=jnp.int32)
    forward = (within[None, None, :] + turns[:, :, None]) % FROWS
    backward = (within[None, None, :] - turns[:, :, None]) % FROWS
    partner_within = jnp.where(upward[None, :, None], forward, backward)
    target = others[:, :, None] * row_count + other_face[:, :, None] * FROWS + partner_within
    inverse = jnp.argsort(shuffle, axis=1).astype(jnp.int32)
    placed = jnp.take_along_axis(target, inverse[:, :, None], axis=1)
    return placed.reshape(SUB_DEV * N_SUB, IF).astype(jnp.int32)


def shard_levels(own_key, extent, pieces, low, largest):
    loudness, own = 1.0, jax.random.fold_in(own_key, 6)
    for position, blocks in pieces:
        steps = jnp.exp(jax.random.uniform(jax.random.fold_in(own, position), (blocks,), jnp.float32, low / len(pieces), largest / len(pieces)))
        loudness = loudness * jnp.repeat(steps, extent[position] // blocks).reshape([-1 if axis == position else 1 for axis in range(len(extent))])
    return loudness


def scatter_about(stream_key, extent, width, reach, shards=(), held_as=jnp.bfloat16):
    entries = width * jax.random.normal(stream_key, extent, jnp.float32)
    if shards:
        entries = entries * shard_levels(stream_key, extent, shards, -0.22, 0.18)
    return jnp.clip(entries, -reach, reach).astype(held_as)


def setup_inputs(seed: int = 0, part: int = 0) -> dict:
    key_of = jax.random.split(jax.random.key(seed), 6)
    own_keys = jax.random.split(jax.random.fold_in(key_of[5], part), 6)
    factors = scatter_about(own_keys[0], (SUBS, NDOF, NDOF), NDOF ** -0.5, 0.1875, ((0, 128),))
    coupling = scatter_about(own_keys[1], (SUBS, NDOF, IF), NDOF ** -0.5, 0.1875, ((0, 128),))
    gap_loads = draw_gap_loads(jax.random.fold_in(jax.random.fold_in(key_of[5], part), 71), part)
    dof_blocks = draw_dof_blocks(jax.random.fold_in(jax.random.fold_in(key_of[5], part), 71), part)
    partner_rows = draw_partner_rows(jax.random.fold_in(jax.random.fold_in(key_of[5], part), 71), part)
    return dict(factors=factors, coupling=coupling, gap_loads=gap_loads, dof_blocks=dof_blocks, partner_rows=partner_rows)


STEP_SIZE = 0.25

def build_panel(inputs):
    factor, couple, blocks = inputs
    present = jnp.arange(factor.shape[0]) < blocks * DBLK
    masked = jnp.where(present[:, None], couple, jnp.zeros_like(couple))
    product = jnp.dot(factor.T, masked, preferred_element_type=jnp.float32)
    reduced = jnp.where(present[:, None], product, jnp.zeros_like(product)).astype(jnp.bfloat16)
    schur_panel = jnp.dot(reduced.T, reduced, preferred_element_type=jnp.float32)
    return schur_panel.astype(jnp.bfloat16)

def reference(factors, coupling, gap_loads, dof_blocks, partner_rows):
    panels = lax.map(build_panel, (factors, coupling, dof_blocks))
    subdomains, interface, load_cases = gap_loads.shape
    partners = partner_rows.reshape(-1).astype(jnp.int32)
    own_rows = jnp.arange(partners.shape[0], dtype=jnp.int32)
    orient = jnp.where(own_rows < partners, 1.0, -1.0).astype(jnp.float32).reshape(subdomains, interface, 1)
    load_values = gap_loads.astype(jnp.float32)

    def pair_add(values):
        flat_values = values.reshape(-1, load_cases)
        return (flat_values + flat_values[partners]).reshape(values.shape)
    residual = pair_add(orient * load_values)
    multipliers = jnp.zeros_like(residual)
    for iteration in range(ITERS):
        multipliers = multipliers + STEP_SIZE * residual
        signed = (orient * multipliers).astype(jnp.bfloat16)
        panel_image = jnp.einsum('sij,sjc->sic', panels.astype(jnp.float32), signed.astype(jnp.float32), precision=lax.Precision.HIGHEST)
        residual = pair_add(orient * (load_values - panel_image))
    squares = lax.optimization_barrier(jnp.mean(residual * residual, axis=(0, 1)))
    return (multipliers, residual, jnp.sqrt(squares + 1e-06))
```

```python
import jax
import jax.numpy as jnp
from jax import lax
from jax.experimental import pallas as pl
from jax.experimental.pallas import tpu as pltpu
from jax.sharding import Mesh
from jax.sharding import PartitionSpec as P

DBLK = 128
FROWS = 16
ITERS = 3
LANES = 128
TILE = 512
SUB = ("sub_0", "sub_1", "sub_2")
GRP_SUB = ("grp", "sub_0", "sub_1", "sub_2")

STEP_SIZE = 0.25
F32 = jnp.float32
BF16 = jnp.bfloat16


def whole_panel(factor, couple, blocks):
    present = jnp.arange(couple.shape[0]) < blocks * DBLK
    masked = jnp.where(present[:, None], couple, jnp.zeros_like(couple))
    product = lax.dot_general(
        factor, masked, (((0,), (0,)), ((), ())), preferred_element_type=F32
    )
    reduced = jnp.where(present[:, None], product, jnp.zeros_like(product)).astype(BF16)
    schur_panel = lax.dot_general(
        reduced, reduced, (((0,), (0,)), ((), ())), preferred_element_type=F32
    )
    return schur_panel.astype(BF16)


def total_over_group(part):
    for axes in (("sub_0",), ("sub_1", "sub_2")):
        copies = jnp.broadcast_to(part[None], (lax.axis_size(axes),) + part.shape)
        part = jnp.sum(lax.all_to_all(copies, axes, 0, 0, tiled=True), axis=0)
    return part


def place_rows(slot_ref, values_ref, send_ref):
    rows = values_ref.shape[0]

    def body(q, carry):
        base = pl.multiple_of(q * TILE, TILE)
        ids = lax.broadcasted_iota(jnp.int32, (TILE, rows), 0) + base
        chosen = jnp.where(ids == slot_ref[...], 1.0, 0.0).astype(BF16)
        placed = jnp.dot(chosen, values_ref[...], preferred_element_type=F32)
        send_ref[pl.ds(base, TILE), :] = placed.astype(BF16)
        return carry

    lax.fori_loop(0, send_ref.shape[0] // TILE, body, 0)


def landed_rows(slot_col_ref, incoming_ref, base):
    slots = incoming_ref.shape[0]
    column = slot_col_ref[pl.ds(base, TILE), :]
    pieces = []
    lane = lax.broadcasted_iota(jnp.int32, (TILE, LANES), 1)
    for t in range(slots // LANES):
        pieces.append(jnp.where(lane + t * LANES == column, 1.0, 0.0).astype(BF16))
    chosen = jnp.concatenate(pieces, axis=1)
    return jnp.dot(chosen, incoming_ref[...], preferred_element_type=F32)


def open_kernel(position_ref, partner_ref, gap_ref, send_ref, slot_ref, order_ref, sign_ref, comp):
    subdomains, interface = partner_ref.shape
    rows = subdomains * interface
    tiles = rows // LANES
    per = interface // LANES
    span = pl.next_power_of_2(rows)
    partner = jnp.concatenate(
        [
            partner_ref[s : s + 1, t * LANES : (t + 1) * LANES]
            for s in range(subdomains)
            for t in range(per)
        ],
        axis=0,
    )
    target = jnp.floor((partner.astype(F32) + 0.5) * (1.0 / rows))
    remote = partner.astype(F32) - target * rows
    ordinal = (
        lax.broadcasted_iota(jnp.int32, (tiles, LANES), 0) * LANES
        + lax.broadcasted_iota(jnp.int32, (tiles, LANES), 1)
    ).astype(F32)
    lower = position_ref[0].astype(F32) < target
    first = target * span
    full = first + jnp.where(lower, ordinal, remote)
    for t in range(tiles):
        comp[t * LANES : (t + 1) * LANES, :] = jnp.broadcast_to(
            full[t : t + 1, :], (LANES, LANES)
        ).T
    ranks = []
    for t in range(tiles):
        lo, hi = first[t : t + 1, :], full[t : t + 1, :]

        def count(j, acc, lo=lo, hi=hi):
            other = comp[pl.ds(pl.multiple_of(j * LANES, LANES), LANES), :]
            ahead = jnp.where((other >= lo) & (other < hi), 1.0, 0.0)
            return acc + jnp.sum(ahead.reshape(LANES // 8, 8, LANES), axis=0)

        acc = lax.fori_loop(0, tiles, count, jnp.zeros((8, LANES), F32))
        ranks.append(jnp.sum(acc, axis=0, keepdims=True))
    slot = (target * FROWS + jnp.concatenate(ranks, axis=0)).astype(jnp.int32)
    order_ref[...] = slot
    sign_ref[...] = jnp.where(lower, 1.0, -1.0)
    for t in range(tiles):
        slot_ref[:, t * LANES : (t + 1) * LANES] = slot[t : t + 1, :]
    place_rows(slot_ref, gap_ref, send_ref)


def step_kernel(incoming_ref, own_ref, mult_ref, gap_ref, panel_ref, slot_ref, slot_col_ref, sign_ref,
                send_ref, own_out, mult_out, own_bf):
    def body(s, carry):
        base = pl.multiple_of(s * TILE, TILE)
        here = pl.ds(base, TILE)
        sign = jnp.concatenate([sign_ref[here, :]] * (own_ref.shape[1] // LANES), axis=1)
        residual = own_ref[here, :] - landed_rows(slot_col_ref, incoming_ref, base)
        mult = mult_ref[here, :] + (STEP_SIZE * sign) * residual
        mult_out[here, :] = mult
        signed = (sign * mult).astype(BF16)
        image = jnp.dot(panel_ref[s], signed, preferred_element_type=F32)
        own = gap_ref[here, :].astype(F32) - image
        own_out[here, :] = own
        own_bf[here, :] = own.astype(BF16)
        return carry

    lax.fori_loop(0, own_ref.shape[0] // TILE, body, 0)
    place_rows(slot_ref, own_bf, send_ref)


def close_kernel(incoming_ref, own_ref, slot_col_ref, sign_ref, residual_ref, squares_ref):
    columns = own_ref.shape[1]

    def body(s, acc):
        base = pl.multiple_of(s * TILE, TILE)
        here = pl.ds(base, TILE)
        sign = jnp.concatenate([sign_ref[here, :]] * (columns // LANES), axis=1)
        residual = own_ref[here, :] - landed_rows(slot_col_ref, incoming_ref, base)
        residual_ref[here, :] = sign * residual
        return acc + jnp.sum((residual * residual).reshape(TILE // 8, 8, columns), axis=0)

    acc = lax.fori_loop(0, own_ref.shape[0] // TILE, body, jnp.zeros((8, columns), F32))
    squares_ref[...] = jnp.sum(acc, axis=0, keepdims=True)


def vmem_call(kernel, outs, n_in, scratch=(), smem_first=False, aliases=None, flops=0):
    spec = pl.BlockSpec(memory_space=pltpu.VMEM)
    in_specs = [spec] * n_in
    if smem_first:
        in_specs[0] = pl.BlockSpec(memory_space=pltpu.SMEM)
    return pl.pallas_call(
        kernel,
        out_shape=[jax.ShapeDtypeStruct(s, d) for s, d in outs],
        in_specs=in_specs,
        out_specs=[spec] * len(outs),
        scratch_shapes=list(scratch),
        input_output_aliases=aliases or {},
        cost_estimate=pl.CostEstimate(flops=flops, bytes_accessed=8 << 20, transcendentals=0),
        compiler_params=pltpu.CompilerParams(vmem_limit_bytes=40 << 20),
    )


def local(factors, coupling, gap_loads, dof_blocks, partner_rows):
    subdomains, interface, columns = gap_loads.shape
    devices = lax.axis_size(SUB)
    position = lax.axis_index(SUB)
    rows = subdomains * interface
    slots = devices * FROWS
    tiles = rows // LANES
    gap = gap_loads.reshape(rows, columns)

    def exchange(outgoing):
        blocks = outgoing.reshape(devices, FROWS, columns)
        return lax.all_to_all(blocks, SUB, split_axis=0, concat_axis=0, tiled=True).reshape(
            slots, columns
        )

    outgoing, slot, order, sign = vmem_call(
        open_kernel,
        [((slots, columns), BF16), ((1, rows), jnp.int32), ((tiles, LANES), jnp.int32), ((tiles, LANES), F32)],
        3,
        scratch=[pltpu.VMEM((rows, LANES), F32)],
        smem_first=True,
        flops=2 * slots * rows * columns,
    )(position.astype(jnp.int32).reshape(1), partner_rows, gap)
    incoming = exchange(outgoing)
    panels = jnp.stack(
        [whole_panel(factors[s], coupling[s], dof_blocks[s]) for s in range(subdomains)]
    )
    slot_col = jnp.broadcast_to(order.reshape(rows, 1), (rows, LANES))
    sign_col = jnp.broadcast_to(sign.reshape(rows, 1), (rows, LANES))
    step = vmem_call(
        step_kernel,
        [((slots, columns), BF16), ((rows, columns), F32), ((rows, columns), F32)],
        8,
        scratch=[pltpu.VMEM((rows, columns), BF16)],
        aliases={1: 1, 2: 2},
        flops=4 * slots * rows * columns,
    )

    def iteration(_, carry):
        incoming, own, multipliers = carry
        outgoing, own, multipliers = step(
            incoming, own, multipliers, gap, panels, slot, slot_col, sign_col
        )
        return exchange(outgoing), own, multipliers

    carry = (incoming, gap.astype(F32), jnp.zeros((rows, columns), F32))
    for k in range(ITERS):
        carry = iteration(k, carry)
    incoming, own, multipliers = carry
    residual, squares = vmem_call(
        close_kernel, [((rows, columns), F32), ((1, columns), F32)], 4, flops=2 * slots * rows * columns
    )(incoming, own, slot_col, sign_col)
    squares = total_over_group(squares).reshape(columns)
    shape = (subdomains, interface, columns)
    return (
        multipliers.reshape(shape),
        residual.reshape(shape),
        jnp.sqrt(squares / (rows * devices) + 1e-06),
    )


def solution(mesh):
    finer = Mesh(
        mesh.devices.reshape(mesh.shape["grp"], 16, 4, 2), ("grp", "sub_0", "sub_1", "sub_2")
    )
    in_specs = (
        P(GRP_SUB, None, None),
        P(GRP_SUB, None, None),
        P(GRP_SUB, None, None),
        P(GRP_SUB),
        P(GRP_SUB, None),
    )
    out_specs = (P(GRP_SUB, None, None), P(GRP_SUB, None, None), P("grp"))
    return jax.shard_map(local, mesh=finer, in_specs=in_specs, out_specs=out_specs, check_vma=False)
```

```python
import functools

import jax
import jax.numpy as jnp
from jax import lax
from jax.experimental import pallas as pl
from jax.experimental.pallas import tpu as pltpu
from jax.sharding import Mesh
from jax.sharding import PartitionSpec as P

DBLK = 128
FROWS = 16
ITERS = 3
LANES = 128
SUBLANES = 8
TILE = 512
SUB = ("sub_0", "sub_1", "sub_2")
GRP_SUB = ("grp", "sub_0", "sub_1", "sub_2")

STEP_SIZE = 0.25
F32 = jnp.float32
BF16 = jnp.bfloat16


def whole_panel(factor, couple, blocks):
    present = jnp.arange(couple.shape[0]) < blocks * DBLK
    masked = jnp.where(present[:, None], couple, jnp.zeros_like(couple))
    product = lax.dot_general(
        factor, masked, (((0,), (0,)), ((), ())), preferred_element_type=F32
    )
    reduced = jnp.where(present[:, None], product, jnp.zeros_like(product)).astype(BF16)
    schur_panel = lax.dot_general(
        reduced, reduced, (((0,), (0,)), ((), ())), preferred_element_type=F32
    )
    return schur_panel.astype(BF16)


def chosen_rows(slot_ref, base, count):
    ids = lax.broadcasted_iota(jnp.int32, (count, slot_ref.shape[1]), 0) + base
    return jnp.where(ids == slot_ref[...], 1.0, 0.0).astype(BF16)


def open_kernel(position_ref, partner_hbm, gap_hbm, send_ref, slot_ref, order_ref, sign_ref, partner_ref, gap_ref, comp, sems):
    load_partner = pltpu.make_async_copy(partner_hbm, partner_ref, sems.at[0])
    load_gap = pltpu.make_async_copy(gap_hbm, gap_ref, sems.at[1])
    load_partner.start()
    load_gap.start()
    load_partner.wait()
    subdomains, interface = partner_ref.shape
    rows = subdomains * interface
    tiles = rows // LANES
    span = pl.next_power_of_2(rows)
    partner = jnp.concatenate(
        [
            partner_ref[s : s + 1, t : t + LANES]
            for s in range(subdomains)
            for t in range(0, interface, LANES)
        ],
        axis=0,
    ).astype(F32)
    target = jnp.floor((partner + 0.5) * (1.0 / rows))
    remote = partner - target * rows
    ordinal = (
        lax.broadcasted_iota(jnp.int32, (tiles, LANES), 0) * LANES
        + lax.broadcasted_iota(jnp.int32, (tiles, LANES), 1)
    ).astype(F32)
    first = target * span
    lower = position_ref[0].astype(F32) < target
    sign_ref[...] = jnp.where(lower, 1.0, -1.0)
    full = first + jnp.where(lower, ordinal, remote)
    for t in range(tiles):
        comp[t * LANES : (t + 1) * LANES, :] = jnp.broadcast_to(
            full[t : t + 1, :], (LANES, LANES)
        ).T
    low = [jnp.broadcast_to(first[t : t + 1, :], (SUBLANES, LANES)) for t in range(tiles)]
    high = [jnp.broadcast_to(full[t : t + 1, :], (SUBLANES, LANES)) for t in range(tiles)]

    def count(j, acc):
        acc = list(acc)
        for k in range(4):
            other = comp[pl.ds(pl.multiple_of(j * 4 * SUBLANES, 4 * SUBLANES) + k * SUBLANES, SUBLANES), :]
            for t in range(tiles):
                acc[t] = acc[t] + jnp.where((other >= low[t]) & (other < high[t]), 1.0, 0.0)
        return tuple(acc)

    zero = jnp.zeros((SUBLANES, LANES), F32)
    acc = lax.fori_loop(0, rows // (4 * SUBLANES), count, (zero,) * tiles)
    for t in range(tiles):
        rank = jnp.sum(acc[t], axis=0, keepdims=True)
        slot = (target[t : t + 1, :] * FROWS + rank).astype(jnp.int32)
        slot_ref[:, t * LANES : (t + 1) * LANES] = slot
        order_ref[t : t + 1, :] = slot
    load_gap.wait()

    def place(q, carry):
        base = pl.multiple_of(q * TILE, TILE)
        placed = jnp.dot(chosen_rows(slot_ref, base, TILE), gap_ref[...], preferred_element_type=F32)
        send_ref[pl.ds(base, TILE), :] = placed.astype(BF16)
        return carry

    lax.fori_loop(0, send_ref.shape[0] // TILE, place, 0)


def build_kernel(slot_ref, panel_ref, matrix_ref, place_ref, half):
    slots, _ = place_ref.shape
    subdomains, interface = panel_ref.shape[:2]

    def choose(q, carry):
        base = pl.multiple_of(q * 256, 256)
        place_ref[pl.ds(base, 256), :] = chosen_rows(slot_ref, base, 256)
        return carry

    lax.fori_loop(0, slots // 256, choose, 0)

    def body(q, carry):
        here = pl.ds(pl.multiple_of(q * TILE, TILE), TILE)
        for s in range(subdomains):
            cols = slice(s * interface, (s + 1) * interface)
            half[:, cols] = jnp.dot(
                place_ref[here, cols], panel_ref[s], preferred_element_type=F32
            ).astype(BF16)
        for n in range(0, slots, 1024):
            matrix_ref[here, n : n + 1024] = lax.dot_general(
                half[...], place_ref[n : n + 1024, :], (((1,), (1,)), ((), ())), preferred_element_type=F32
            ).astype(BF16)
        return carry

    lax.fori_loop(0, slots // TILE, body, 0)


def step_kernel(*refs, first, last):
    if first:
        incoming_ref, gap_ref, matrix_ref, send_ref, next_ref, signed_ref = refs
    elif last:
        base_ref, incoming_ref, gap_ref, matrix_ref, send_ref, signed_ref = refs
    else:
        base_ref, incoming_ref, gap_ref, matrix_ref, send_ref, next_ref, signed_ref = refs

    def multipliers(here):
        base = STEP_SIZE * gap_ref[here, :].astype(F32) if first else base_ref[here, :]
        return base - STEP_SIZE * incoming_ref[here, :].astype(F32)

    tiles = [slice(q, q + TILE) for q in range(0, send_ref.shape[0], TILE)]
    for here in tiles:
        signed_ref[here, :] = multipliers(here).astype(BF16)
    for here in tiles:
        image = jnp.dot(matrix_ref[here, :], signed_ref[...], preferred_element_type=F32)
        own = gap_ref[here, :].astype(F32) - image
        send_ref[here, :] = own.astype(BF16)
        if not last:
            next_ref[here, :] = multipliers(here) + STEP_SIZE * own


def chosen_slots(column_ref, base, slots):
    column = column_ref[pl.ds(base, TILE), :]
    lane = lax.broadcasted_iota(jnp.int32, (TILE, LANES), 1)
    pieces = [
        jnp.where(lane + t == column, 1.0, 0.0).astype(BF16) for t in range(0, slots, LANES)
    ]
    return jnp.concatenate(pieces, axis=1)


def across(sign_ref, here, columns):
    return jnp.concatenate([sign_ref[here, :]] * (columns // LANES), axis=1)


def last_kernel(base_ref, incoming_ref, gap_ref, column_ref, sign_ref, panel_ref,
                own_ref, mult_ref, signed, low):
    slots, columns = signed.shape

    def split(q, carry):
        here = pl.ds(pl.multiple_of(q * TILE, TILE), TILE)
        value = base_ref[here, :] - STEP_SIZE * incoming_ref[here, :].astype(F32)
        high = value.astype(BF16)
        signed[here, :] = high
        low[here, :] = (value - high.astype(F32)).astype(BF16)
        return carry

    lax.fori_loop(0, slots // TILE, split, 0)

    def rows(s, carry):
        base = pl.multiple_of(s * TILE, TILE)
        here = pl.ds(base, TILE)
        chosen = chosen_slots(column_ref, base, slots)
        high = jnp.dot(chosen, signed[...], preferred_element_type=F32)
        rest = jnp.dot(chosen, low[...], preferred_element_type=F32)
        mult_ref[here, :] = across(sign_ref, here, columns) * (high + rest)
        image = jnp.dot(panel_ref[s], high.astype(BF16), preferred_element_type=F32)
        own_ref[here, :] = gap_ref[here, :].astype(F32) - image
        return carry

    lax.fori_loop(0, panel_ref.shape[0], rows, 0)


def close_kernel(own_ref, incoming_ref, column_ref, sign_ref, residual_ref, squares_ref):
    slots, columns = incoming_ref.shape

    def body(s, acc):
        base = pl.multiple_of(s * TILE, TILE)
        here = pl.ds(base, TILE)
        landed = jnp.dot(
            chosen_slots(column_ref, base, slots), incoming_ref[...], preferred_element_type=F32
        )
        residual = own_ref[here, :] - landed
        residual_ref[here, :] = across(sign_ref, here, columns) * residual
        return acc + jnp.sum((residual * residual).reshape(TILE // SUBLANES, SUBLANES, columns), axis=0)

    acc = lax.fori_loop(0, own_ref.shape[0] // TILE, body, jnp.zeros((SUBLANES, columns), F32))
    squares_ref[...] = jnp.sum(acc, axis=0, keepdims=True)


VMEM = pl.BlockSpec(memory_space=pltpu.VMEM)
SMEM = pl.BlockSpec(memory_space=pltpu.SMEM)
ANY = pl.BlockSpec(memory_space=pl.ANY)


def call(kernel, outs, in_specs, scratch=(), flops=0, limit=24):
    return pl.pallas_call(
        kernel,
        out_shape=[jax.ShapeDtypeStruct(s, d) for s, d in outs],
        in_specs=in_specs,
        out_specs=[VMEM] * len(outs),
        scratch_shapes=list(scratch),
        cost_estimate=pl.CostEstimate(flops=flops, bytes_accessed=8 << 20, transcendentals=0),
        compiler_params=pltpu.CompilerParams(vmem_limit_bytes=limit << 20),
    )


def local(factors, coupling, gap_loads, dof_blocks, partner_rows):
    subdomains, interface, columns = gap_loads.shape
    devices = lax.axis_size(SUB)
    position = lax.axis_index(SUB).astype(jnp.int32).reshape(1)
    rows = subdomains * interface
    slots = devices * FROWS
    place_flops = 2 * slots * rows * columns
    matrix_flops = 2 * slots * slots * columns

    def exchange(outgoing):
        blocks = outgoing.reshape(devices, FROWS, columns)
        incoming = lax.all_to_all(blocks, SUB, split_axis=0, concat_axis=0, tiled=True)
        return incoming.reshape(slots, columns)

    flat = gap_loads.reshape(rows, columns)
    gap, slot, order, sign = call(
        open_kernel,
        [
            ((slots, columns), BF16),
            ((1, rows), jnp.int32),
            ((rows // LANES, LANES), jnp.int32),
            ((rows // LANES, LANES), F32),
        ],
        [SMEM, ANY, ANY],
        [
            pltpu.VMEM(partner_rows.shape, jnp.int32),
            pltpu.VMEM((rows, columns), BF16),
            pltpu.VMEM((rows, LANES), F32),
            pltpu.SemaphoreType.DMA((2,)),
        ],
        flops=place_flops,
        limit=60,
    )(position, partner_rows, flat)
    incoming = exchange(gap)
    panels = jnp.stack(
        [whole_panel(factors[s], coupling[s], dof_blocks[s]) for s in range(subdomains)]
    )
    (matrix,) = call(
        build_kernel,
        [((slots, slots), BF16)],
        [VMEM] * 2,
        [pltpu.VMEM((slots, rows), BF16), pltpu.VMEM((TILE, rows), BF16)],
        flops=2 * slots * rows * slots,
        limit=28,
    )(slot, panels)
    column = jnp.broadcast_to(order.reshape(rows, 1), (rows, LANES))
    sign = jnp.broadcast_to(sign.reshape(rows, 1), (rows, LANES))
    state = ()
    for k in range(1, ITERS + 1):
        first, last = k == 1, k == ITERS
        outgoing, *following = call(
            functools.partial(step_kernel, first=first, last=last),
            [((slots, columns), BF16)] + [((slots, columns), F32)] * (not last),
            [VMEM] * (len(state) + 3),
            [pltpu.VMEM((slots, columns), BF16)],
            flops=matrix_flops,
            limit=20,
        )(*state, incoming, gap, matrix)
        arriving = exchange(outgoing)
        if last:
            own, multipliers = call(
                last_kernel,
                [((rows, columns), F32)] * 2,
                [VMEM] * 6,
                [pltpu.VMEM((slots, columns), BF16)] * 2,
                flops=3 * place_flops,
                limit=34,
            )(*state, incoming, flat, column, sign, panels)
        incoming, state = arriving, following
    residual, squares = call(
        close_kernel,
        [((rows, columns), F32), ((1, columns), F32)],
        [VMEM] * 4,
        flops=place_flops,
        limit=20,
    )(own, incoming, column, sign)
    for axes in (("sub_0",), ("sub_1", "sub_2")):
        copies = jnp.broadcast_to(squares[None], (lax.axis_size(axes),) + squares.shape)
        parts = lax.all_to_all(copies, axes, 0, 0, tiled=True)
        squares = jnp.sum(parts, axis=0)
    shape = (subdomains, interface, columns)
    return (
        multipliers.reshape(shape),
        residual.reshape(shape),
        jnp.sqrt(squares.reshape(columns) / (rows * devices) + 1e-06),
    )


def solution(mesh):
    finer = Mesh(
        mesh.devices.reshape(mesh.shape["grp"], 16, 4, 2), ("grp", "sub_0", "sub_1", "sub_2")
    )
    in_specs = (
        P(GRP_SUB, None, None),
        P(GRP_SUB, None, None),
        P(GRP_SUB, None, None),
        P(GRP_SUB),
        P(GRP_SUB, None),
    )
    out_specs = (P(GRP_SUB, None, None), P(GRP_SUB, None, None), P("grp"))
    return jax.shard_map(local, mesh=finer, in_specs=in_specs, out_specs=out_specs, check_vma=False)
```

```python
import functools

import jax
import jax.numpy as jnp
from jax import lax
from jax.experimental import pallas as pl
from jax.experimental.pallas import tpu as pltpu
from jax.sharding import Mesh
from jax.sharding import PartitionSpec as P

DBLK = 128
FROWS = 16
ITERS = 3
LANES = 128
SUBLANES = 8
TILE = 512
SUB = ("sub_0", "sub_1", "sub_2")
GRP_SUB = ("grp", "sub_0", "sub_1", "sub_2")

STEP_SIZE = 0.25
F32 = jnp.float32
BF16 = jnp.bfloat16


def whole_panel(factor, couple, blocks):
    present = jnp.arange(couple.shape[0]) < blocks * DBLK
    masked = jnp.where(present[:, None], couple, jnp.zeros_like(couple))
    product = lax.dot_general(
        factor, masked, (((0,), (0,)), ((), ())), preferred_element_type=F32
    )
    reduced = jnp.where(present[:, None], product, jnp.zeros_like(product)).astype(BF16)
    schur_panel = lax.dot_general(
        reduced, reduced, (((0,), (0,)), ((), ())), preferred_element_type=F32
    )
    return schur_panel.astype(BF16)


def chosen_rows(slot_ref, base, count):
    ids = lax.broadcasted_iota(jnp.int32, (count, slot_ref.shape[1]), 0) + base
    return jnp.where(ids == slot_ref[...], 1.0, 0.0).astype(BF16)


def open_kernel(position_ref, partner_hbm, gap_hbm, send_ref, slot_ref, order_ref, partner_ref, gap_ref, comp, sems):
    load_partner = pltpu.make_async_copy(partner_hbm, partner_ref, sems.at[0])
    load_gap = pltpu.make_async_copy(gap_hbm, gap_ref, sems.at[1])
    load_partner.start()
    load_gap.start()
    load_partner.wait()
    subdomains, interface = partner_ref.shape
    rows = subdomains * interface
    tiles = rows // LANES
    span = pl.next_power_of_2(rows)
    partner = jnp.concatenate(
        [
            partner_ref[s : s + 1, t : t + LANES]
            for s in range(subdomains)
            for t in range(0, interface, LANES)
        ],
        axis=0,
    ).astype(F32)
    target = jnp.floor((partner + 0.5) * (1.0 / rows))
    remote = partner - target * rows
    ordinal = (
        lax.broadcasted_iota(jnp.int32, (tiles, LANES), 0) * LANES
        + lax.broadcasted_iota(jnp.int32, (tiles, LANES), 1)
    ).astype(F32)
    first = target * span
    full = first + jnp.where(position_ref[0].astype(F32) < target, ordinal, remote)
    for t in range(tiles):
        comp[t * LANES : (t + 1) * LANES, :] = jnp.broadcast_to(
            full[t : t + 1, :], (LANES, LANES)
        ).T
    low = [jnp.broadcast_to(first[t : t + 1, :], (SUBLANES, LANES)) for t in range(tiles)]
    high = [jnp.broadcast_to(full[t : t + 1, :], (SUBLANES, LANES)) for t in range(tiles)]

    def count(j, acc):
        acc = list(acc)
        for k in range(4):
            other = comp[pl.ds(pl.multiple_of(j * 4 * SUBLANES, 4 * SUBLANES) + k * SUBLANES, SUBLANES), :]
            for t in range(tiles):
                acc[t] = acc[t] + jnp.where((other >= low[t]) & (other < high[t]), 1.0, 0.0)
        return tuple(acc)

    zero = jnp.zeros((SUBLANES, LANES), F32)
    acc = lax.fori_loop(0, rows // (4 * SUBLANES), count, (zero,) * tiles)
    for t in range(tiles):
        rank = jnp.sum(acc[t], axis=0, keepdims=True)
        slot = (target[t : t + 1, :] * FROWS + rank).astype(jnp.int32)
        slot_ref[:, t * LANES : (t + 1) * LANES] = slot
        order_ref[t : t + 1, :] = slot
    load_gap.wait()

    def place(q, carry):
        base = pl.multiple_of(q * TILE, TILE)
        placed = jnp.dot(chosen_rows(slot_ref, base, TILE), gap_ref[...], preferred_element_type=F32)
        send_ref[pl.ds(base, TILE), :] = placed.astype(BF16)
        return carry

    lax.fori_loop(0, send_ref.shape[0] // TILE, place, 0)


def build_kernel(slot_ref, panel_ref, matrix_ref, place_ref, half):
    slots, _ = place_ref.shape
    subdomains, interface = panel_ref.shape[:2]

    def choose(q, carry):
        base = pl.multiple_of(q * 256, 256)
        place_ref[pl.ds(base, 256), :] = chosen_rows(slot_ref, base, 256)
        return carry

    lax.fori_loop(0, slots // 256, choose, 0)

    def body(q, carry):
        here = pl.ds(pl.multiple_of(q * TILE, TILE), TILE)
        for s in range(subdomains):
            cols = slice(s * interface, (s + 1) * interface)
            half[:, cols] = jnp.dot(
                place_ref[here, cols], panel_ref[s], preferred_element_type=F32
            ).astype(BF16)
        for n in range(0, slots, 1024):
            matrix_ref[here, n : n + 1024] = lax.dot_general(
                half[...], place_ref[n : n + 1024, :], (((1,), (1,)), ((), ())), preferred_element_type=F32
            ).astype(BF16)
        return carry

    lax.fori_loop(0, slots // TILE, body, 0)


def step_kernel(*refs, first, last):
    if first:
        incoming_ref, gap_ref, matrix_ref, send_ref, next_ref, signed_ref = refs
    elif last:
        base_ref, incoming_ref, gap_ref, matrix_ref, send_ref, signed_ref = refs
    else:
        base_ref, incoming_ref, gap_ref, matrix_ref, send_ref, next_ref, signed_ref = refs

    def multipliers(here):
        base = STEP_SIZE * gap_ref[here, :].astype(F32) if first else base_ref[here, :]
        return base - STEP_SIZE * incoming_ref[here, :].astype(F32)

    tiles = [slice(q, q + TILE) for q in range(0, send_ref.shape[0], TILE)]
    for here in tiles:
        signed_ref[here, :] = multipliers(here).astype(BF16)
    for here in tiles:
        image = jnp.dot(matrix_ref[here, :], signed_ref[...], preferred_element_type=F32)
        own = gap_ref[here, :].astype(F32) - image
        send_ref[here, :] = own.astype(BF16)
        if not last:
            next_ref[here, :] = multipliers(here) + STEP_SIZE * own


def chosen_slots(column_ref, base, slots):
    column = column_ref[pl.ds(base, TILE), :]
    lane = lax.broadcasted_iota(jnp.int32, (TILE, LANES), 1)
    pieces = [
        jnp.where(lane + t == column, 1.0, 0.0).astype(BF16) for t in range(0, slots, LANES)
    ]
    return jnp.concatenate(pieces, axis=1)


def orient(position_ref, column_ref, here, columns):
    after = column_ref[here, :] >= (position_ref[0] + 1) * FROWS
    return jnp.concatenate([jnp.where(after, 1.0, -1.0)] * (columns // LANES), axis=1)


def last_kernel(position_ref, base_ref, incoming_ref, gap_ref, column_ref, panel_ref,
                own_ref, mult_ref, signed, low):
    slots, columns = signed.shape

    def split(q, carry):
        here = pl.ds(pl.multiple_of(q * TILE, TILE), TILE)
        value = base_ref[here, :] - STEP_SIZE * incoming_ref[here, :].astype(F32)
        high = value.astype(BF16)
        signed[here, :] = high
        low[here, :] = (value - high.astype(F32)).astype(BF16)
        return carry

    lax.fori_loop(0, slots // TILE, split, 0)

    def rows(s, carry):
        base = pl.multiple_of(s * TILE, TILE)
        here = pl.ds(base, TILE)
        chosen = chosen_slots(column_ref, base, slots)
        high = jnp.dot(chosen, signed[...], preferred_element_type=F32)
        rest = jnp.dot(chosen, low[...], preferred_element_type=F32)
        mult_ref[here, :] = orient(position_ref, column_ref, here, columns) * (high + rest)
        image = jnp.dot(panel_ref[s], high.astype(BF16), preferred_element_type=F32)
        own_ref[here, :] = gap_ref[here, :].astype(F32) - image
        return carry

    lax.fori_loop(0, panel_ref.shape[0], rows, 0)


def close_kernel(position_ref, own_ref, incoming_ref, column_ref, residual_ref, squares_ref):
    slots, columns = incoming_ref.shape

    def body(s, acc):
        base = pl.multiple_of(s * TILE, TILE)
        here = pl.ds(base, TILE)
        landed = jnp.dot(
            chosen_slots(column_ref, base, slots), incoming_ref[...], preferred_element_type=F32
        )
        residual = own_ref[here, :] - landed
        residual_ref[here, :] = orient(position_ref, column_ref, here, columns) * residual
        return acc + jnp.sum((residual * residual).reshape(TILE // SUBLANES, SUBLANES, columns), axis=0)

    acc = lax.fori_loop(0, own_ref.shape[0] // TILE, body, jnp.zeros((SUBLANES, columns), F32))
    squares_ref[...] = jnp.sum(acc, axis=0, keepdims=True)


VMEM = pl.BlockSpec(memory_space=pltpu.VMEM)
SMEM = pl.BlockSpec(memory_space=pltpu.SMEM)
ANY = pl.BlockSpec(memory_space=pl.ANY)


def call(kernel, outs, in_specs, scratch=(), flops=0, limit=24):
    return pl.pallas_call(
        kernel,
        out_shape=[jax.ShapeDtypeStruct(s, d) for s, d in outs],
        in_specs=in_specs,
        out_specs=[VMEM] * len(outs),
        scratch_shapes=list(scratch),
        cost_estimate=pl.CostEstimate(flops=flops, bytes_accessed=8 << 20, transcendentals=0),
        compiler_params=pltpu.CompilerParams(vmem_limit_bytes=limit << 20),
    )


def local(factors, coupling, gap_loads, dof_blocks, partner_rows):
    subdomains, interface, columns = gap_loads.shape
    devices = lax.axis_size(SUB)
    position = lax.axis_index(SUB).astype(jnp.int32).reshape(1)
    rows = subdomains * interface
    slots = devices * FROWS
    place_flops = 2 * slots * rows * columns
    matrix_flops = 2 * slots * slots * columns

    def exchange(outgoing):
        blocks = outgoing.reshape(devices, FROWS, columns)
        incoming = lax.all_to_all(blocks, SUB, split_axis=0, concat_axis=0, tiled=True)
        return incoming.reshape(slots, columns)

    flat = gap_loads.reshape(rows, columns)
    gap, slot, order = call(
        open_kernel,
        [
            ((slots, columns), BF16),
            ((1, rows), jnp.int32),
            ((rows // LANES, LANES), jnp.int32),
        ],
        [SMEM, ANY, ANY],
        [
            pltpu.VMEM(partner_rows.shape, jnp.int32),
            pltpu.VMEM((rows, columns), BF16),
            pltpu.VMEM((rows, LANES), F32),
            pltpu.SemaphoreType.DMA((2,)),
        ],
        flops=place_flops,
        limit=60,
    )(position, partner_rows, flat)
    incoming = exchange(gap)
    panels = jnp.stack(
        [whole_panel(factors[s], coupling[s], dof_blocks[s]) for s in range(subdomains)]
    )
    (matrix,) = call(
        build_kernel,
        [((slots, slots), BF16)],
        [VMEM] * 2,
        [pltpu.VMEM((slots, rows), BF16), pltpu.VMEM((TILE, rows), BF16)],
        flops=2 * slots * rows * slots,
        limit=28,
    )(slot, panels)
    column = jnp.broadcast_to(order.reshape(rows, 1), (rows, LANES))
    state = ()
    for k in range(1, ITERS + 1):
        first, last = k == 1, k == ITERS
        outgoing, *following = call(
            functools.partial(step_kernel, first=first, last=last),
            [((slots, columns), BF16)] + [((slots, columns), F32)] * (not last),
            [VMEM] * (len(state) + 3),
            [pltpu.VMEM((slots, columns), BF16)],
            flops=matrix_flops,
            limit=20,
        )(*state, incoming, gap, matrix)
        arriving = exchange(outgoing)
        if last:
            own, multipliers = call(
                last_kernel,
                [((rows, columns), F32)] * 2,
                [SMEM] + [VMEM] * 5,
                [pltpu.VMEM((slots, columns), BF16)] * 2,
                flops=3 * place_flops,
                limit=34,
            )(position, *state, incoming, flat, column, panels)
        incoming, state = arriving, following
    residual, squares = call(
        close_kernel,
        [((rows, columns), F32), ((1, columns), F32)],
        [SMEM] + [VMEM] * 3,
        flops=place_flops,
        limit=20,
    )(position, own, incoming, column)
    for axes in (("sub_0",), ("sub_1", "sub_2")):
        copies = jnp.broadcast_to(squares[None], (lax.axis_size(axes),) + squares.shape)
        parts = lax.all_to_all(copies, axes, 0, 0, tiled=True)
        squares = jnp.sum(parts, axis=0)
    shape = (subdomains, interface, columns)
    return (
        multipliers.reshape(shape),
        residual.reshape(shape),
        jnp.sqrt(squares.reshape(columns) / (rows * devices) + 1e-06),
    )


def solution(mesh):
    finer = Mesh(
        mesh.devices.reshape(mesh.shape["grp"], 16, 4, 2), ("grp", "sub_0", "sub_1", "sub_2")
    )
    in_specs = (
        P(GRP_SUB, None, None),
        P(GRP_SUB, None, None),
        P(GRP_SUB, None, None),
        P(GRP_SUB),
        P(GRP_SUB, None),
    )
    out_specs = (P(GRP_SUB, None, None), P(GRP_SUB, None, None), P("grp"))
    return jax.shard_map(local, mesh=finer, in_specs=in_specs, out_specs=out_specs, check_vma=False)
```
